32 devices in a mesh: expert: 4 (over z), tensor: 4 (over y, x), dp: 2 (over core).
Axes of the slice: x: 2, y: 2, z: 4, core: 2. Of those that a mesh axis runs over, the one named last changes fastest.
Arguments:
- hidden_in: bfloat16 [2, 512, 4096], P('dp', 'expert'), may hold values from -64 to 64
- expert_ids: int32 [2, 512, 2], P('dp', 'expert'), may hold values from 0 to 3, all different within a row; in each aligned block of 128 rows (0 to 127, 128 to 255, ..., all dimensions but the last counted through in order) at most 72 rows name the same one
- ffn_gain: float32 [4096], replicated, may hold values from 0.5 to 1.5
- w_router: bfloat16 [4096, 4], replicated, may hold values from -0.09375 to 0.09375
- w_gate: bfloat16 [4, 4096, 14336], P('expert', None, ('tensor', 'dp')), may hold values from -0.09375 to 0.09375
- w_up: bfloat16 [4, 4096, 14336], P('expert', None, ('tensor', 'dp')), may hold values from -0.09375 to 0.09375
- w_down: bfloat16 [4, 14336, 4096], P('expert', ('tensor', 'dp')), may hold values from -0.046875 to 0.046875
Outputs:
- hidden_out: bfloat16 [2, 512, 4096], P('dp', 'expert', 'tensor')
- layer_score: float32 [], replicated
The draws below stay inside these ranges and needn't reach their ends.
Inputs may be any that keep to these rules, and one draw needn't show every extreme that they name: `expert_ids`: among the 128 tokens of one device (aligned blocks of the flattened sequence and position order), no expert is chosen by more than 72 of them; a token's two experts differ.
All inputs are finite; a program needn't handle non-finite values.
Results may differ from the reference program's by a relative error of at most 0.0027.
Values may be sent and summed in bfloat16 or wider, within the bound.
No kernel may reach another device: no remote copies, remote signals or barrier semaphores. Data moves between devices by JAX's collectives and lax.ppermute only.
A program may use at most 128 MiB of HBM per device.

```python
import math
import jax
import jax.numpy as jnp
import numpy as np
from jax import lax

D = 4096
FF = 14336
TOP = 2
LEN = 512
EXPERTS = 4
SEQS = 2
TOK_DEV = 128
CAP = 72


def draw_hidden_in(key, part):
    key_base, key_jitter, key_columns = jax.random.split(key, 3)
    token_count = SEQS * LEN
    flat_index = jnp.arange(token_count, dtype=jnp.int32)
    position_frac = (flat_index % LEN).astype(jnp.float32) / (LEN - 1)
    sequence_frac = (flat_index // LEN).astype(jnp.float32) / max(SEQS - 1, 1)
    place = 0.75 * position_frac + 0.25 * sequence_frac
    jitter = jax.random.uniform(key_jitter, (token_count,), jnp.float32, 0.0, 1.0)
    row_scale = jnp.exp(jnp.log(0.5) + jnp.log(8.0) * place + 0.4 * (jitter - 0.5))
    column_scale = jnp.exp(jax.random.uniform(key_columns, (D,), jnp.float32, jnp.log(0.3), jnp.log(3.0)))
    base_draw = jax.random.normal(key_base, (token_count, D), jnp.float32)
    values = jnp.clip(base_draw * row_scale[:, None] * column_scale[None, :], -64.0, 64.0)
    return values.reshape(SEQS, LEN, D).astype(jnp.bfloat16)


def level_of(key, shape, pieces, smallest, top_value):
    factor_of, own = 1.0, jax.random.fold_in(key, 6)
    for axis_at, parts in pieces:
        steps = jnp.exp(jax.random.uniform(jax.random.fold_in(own, axis_at), (parts,), jnp.float32, smallest / len(pieces), top_value / len(pieces)))
        factor_of = factor_of * jnp.repeat(steps, shape[axis_at] // parts).reshape([-1 if axis == axis_at else 1 for axis in range(len(shape))])
    return factor_of


def deal_out(own_key, own, number, rows, number_of, top, reach, slope):
    sequence = jax.random.permutation(own_key, number_of)
    crowded, usual = portions_of(number_of, rows * top, reach, slope, True), portions_of(number_of, rows * top, reach, slope, False)
    places = jnp.arange(number_of)

    def named(lengths, rotation):
        used = int((lengths > 0).sum())
        fixed = max(1, used // 4)
        moved = fixed + (places - fixed + rotation * (used - fixed)) % max(1, number_of - fixed)
        return jnp.zeros((number_of,), jnp.int32).at[sequence[jnp.where(places < fixed, places, moved)]].set(jnp.asarray(lengths, jnp.int32))

    lengths = jnp.where(number % 4 == 0, named(crowded, number // 4), named(usual, number - number // 4 - 1))
    mixed = jax.random.permutation(jax.random.fold_in(own, 3), number_of)
    source_of, sink = mixed[0:number_of // 2 * 2:2], mixed[1:number_of // 2 * 2:2]
    room = jnp.minimum(lengths[source_of] - 1, reach - lengths[sink]) // 2
    room = jnp.where((source_of == sequence[0]) | (sink == sequence[0]) | (lengths[sink] == 0), 0, jnp.maximum(room, 0))
    moved = jax.random.randint(jax.random.fold_in(own, 4), (number_of // 2,), 0, 1 << 20) % (room + 1)
    lengths = lengths.at[source_of].add(-moved).at[sink].add(moved)
    members = jnp.searchsorted(jnp.cumsum(lengths), jnp.arange(rows * top), side="right").astype(jnp.int32)
    grid = members.reshape(top, rows).T
    grid = grid[jax.random.permutation(jax.random.fold_in(own, 1), rows)]
    rotation = jax.random.randint(jax.random.fold_in(own, 2), (rows, 1), 0, top)
    return jnp.take_along_axis(grid, (jnp.arange(top)[None, :] + rotation) % top, axis=1)


def portions_of(number_of, total, limit, slope, full):
    portions = [(1 << 20) // math.isqrt(grade ** slope) + 1 for grade in range(1, number_of + 1)]
    largest = limit if full else min(limit, max(-(-total // number_of), total * portions[0] // sum(portions)))
    least = 1 if total - largest >= number_of - 1 else 0
    counts, spare = [largest] + [least] * (number_of - 1), total - largest - least * (number_of - 1)
    while spare > 0:
        movable = [i for i in range(1, number_of) if counts[i] < largest] or [i for i in range(1, number_of) if counts[i] < limit]
        whole, left = sum([portions[i] for i in movable]), spare
        for i in movable:
            more = min(limit - counts[i], max(1, left * portions[i] // whole), spare)
            counts[i] = counts[i] + more
            spare = spare - more
    return np.array(counts)


def gaussian(rng, dims, scale, bound, shards=(), kind=jnp.bfloat16):
    entries = scale * jax.random.normal(rng, dims, jnp.float32)
    if shards:
        entries = entries * level_of(rng, dims, shards, -0.22, 0.18)
    return jnp.clip(entries, -bound, bound).astype(kind)


def setup_inputs(seed: int = 0) -> dict:
    streams_of = jax.random.split(jax.random.key(seed), 8)
    hidden_in = draw_hidden_in(jax.random.fold_in(streams_of[7], 71), 0)
    expert_ids_keys = jax.random.split(jax.random.fold_in(streams_of[1], 1), SEQS * LEN // TOK_DEV)
    expert_ids_turns = jax.random.permutation(jax.random.fold_in(streams_of[1], 3), SEQS * LEN // TOK_DEV)
    expert_ids = jax.vmap(lambda own, number: deal_out(jax.random.fold_in(streams_of[1], 2), own, number, TOK_DEV, EXPERTS, TOP, CAP, 1))(expert_ids_keys, expert_ids_turns).reshape((SEQS, LEN, TOP))
    ffn_gain = jnp.clip(1.0 + 0.1 * jax.random.normal(streams_of[2], (D,), jnp.float32), 0.5, 1.5)
    w_router = gaussian(streams_of[3], (D, EXPERTS), D ** -0.5, 0.09375)
    w_gate = gaussian(streams_of[4], (EXPERTS, D, FF), D ** -0.5, 0.09375, ((0, 4), (2, 8)))
    w_up = gaussian(streams_of[5], (EXPERTS, D, FF), D ** -0.5, 0.09375, ((0, 4), (2, 8)))
    w_down = gaussian(streams_of[6], (EXPERTS, FF, D), FF ** -0.5, 0.046875, ((0, 4), (1, 8)))
    return dict(hidden_in=hidden_in, expert_ids=expert_ids, ffn_gain=ffn_gain, w_router=w_router, w_gate=w_gate, w_up=w_up, w_down=w_down)


EPS_NORM = 1e-05
EPS_COS = 1e-06

def slot_positions(flat_ids):
    pair_count = flat_ids.shape[0]
    onehot = (flat_ids[:, None] == jnp.arange(EXPERTS, dtype=jnp.int32)[None, :]).astype(jnp.int32)
    positions = jnp.arange(pair_count, dtype=jnp.int32)
    earlier = (positions[None, :] < positions[:, None]).astype(jnp.int32)
    before = lax.optimization_barrier(jnp.sum(earlier[:, :, None] * onehot[None, :, :], axis=1))
    return lax.optimization_barrier(jnp.sum(before * onehot, axis=1)).astype(jnp.int32)

def reference(hidden_in, expert_ids, ffn_gain, w_router, w_gate, w_up, w_down):
    token_count = SEQS * LEN
    blocks = token_count // TOK_DEV
    token_rows = hidden_in.reshape(token_count, D).astype(jnp.float32)
    inverse_rms = lax.rsqrt(lax.optimization_barrier(jnp.mean(token_rows * token_rows, axis=1, keepdims=True)) + EPS_NORM)
    normed = (token_rows * inverse_rms * ffn_gain[None, :]).astype(jnp.bfloat16)
    logits = jnp.dot(normed, w_router, preferred_element_type=jnp.float32)
    chosen = expert_ids.reshape(token_count, TOP).astype(jnp.int32)
    selector = (chosen[:, :, None] == jnp.arange(EXPERTS, dtype=jnp.int32)[None, None, :]).astype(jnp.float32)
    picked = lax.optimization_barrier(jnp.sum(selector * logits[:, None, :], axis=2))
    spread = picked[:, 0] - picked[:, 1]
    gate_values = jnp.stack([jax.nn.sigmoid(spread), jax.nn.sigmoid(-spread)], axis=1)
    slot_index = lax.map(slot_positions, chosen.reshape(blocks, TOK_DEV * TOP)).reshape(token_count, TOP)
    block_of = (jnp.arange(token_count, dtype=jnp.int32) // TOK_DEV)[:, None]
    places = (chosen * (blocks * CAP) + block_of * CAP + slot_index).reshape(-1).astype(jnp.int32)
    sources = jnp.broadcast_to(jnp.arange(token_count, dtype=jnp.int32)[:, None], (token_count, TOP)).reshape(-1)
    slot_table = jnp.full((EXPERTS * blocks * CAP,), token_count, dtype=jnp.int32).at[places].set(sources)
    slot_table = slot_table.reshape(EXPERTS, blocks * CAP)
    padded = jnp.concatenate([normed, jnp.zeros((1, D), jnp.bfloat16)], axis=0)

    def run_expert(operands):
        table_row, gate_matrix, up_matrix, down_matrix = operands
        inputs = padded[table_row]
        gate_term = jnp.dot(inputs, gate_matrix, preferred_element_type=jnp.float32)
        up_term = jnp.dot(inputs, up_matrix, preferred_element_type=jnp.float32)
        act = (jax.nn.silu(gate_term) * up_term).astype(jnp.bfloat16)
        return jnp.dot(act, down_matrix, preferred_element_type=jnp.float32).astype(jnp.bfloat16)
    results = lax.map(run_expert, (slot_table, w_gate, w_up, w_down))
    flat_results = results.reshape(EXPERTS * blocks * CAP, D)
    routed = flat_results[places].reshape(token_count, TOP, D).astype(jnp.float32)
    mixture = lax.optimization_barrier(jnp.sum(gate_values[:, :, None] * routed, axis=1))
    outputs = (token_rows + mixture).astype(jnp.bfloat16)
    out_rows = outputs.astype(jnp.float32)
    cosine = lax.optimization_barrier(jnp.mean(token_rows * out_rows, axis=1)) * lax.rsqrt((lax.optimization_barrier(jnp.mean(token_rows * token_rows, axis=1)) + EPS_COS) * (lax.optimization_barrier(jnp.mean(out_rows * out_rows, axis=1)) + EPS_COS))
    layer_score = jnp.mean(1.0 - cosine)
    return (outputs.reshape(SEQS, LEN, D), layer_score)
```

```python
import functools
import jax
import jax.numpy as jnp
from jax import lax
from jax.experimental import pallas as pl
from jax.experimental.pallas import tpu as pltpu
from jax.sharding import PartitionSpec as P

EPS_NORM = 1e-05
EPS_COS = 1e-06


def slot_positions(flat_ids, experts):
    pair_count = flat_ids.shape[0]
    onehot = (flat_ids[:, None] == jnp.arange(experts, dtype=jnp.int32)[None, :]).astype(jnp.int32)
    positions = jnp.arange(pair_count, dtype=jnp.int32)
    earlier = (positions[None, :] < positions[:, None]).astype(jnp.int32)
    before = jnp.sum(earlier[:, :, None] * onehot[None, :, :], axis=1)
    return jnp.sum(before * onehot, axis=1)


def swap(value, axis, step):
    count = lax.axis_size(axis)
    return lax.ppermute(value, axis, [(i, i ^ step) for i in range(count)])


def tile_of(size, most):
    for tile in range(most, 127, -128):
        if size % tile == 0:
            return tile
    return size


def expert_kernel(groups, shares, f_tiles, t_ref, *refs):
    sources = refs[:groups]
    w_gate, w_up, w_down = refs[groups : groups + 3]
    results = refs[groups + 3 : 2 * groups + 3]
    rows_ref, act_ref, sems = refs[2 * groups + 3 :]
    step = pl.program_id(0)
    rows = sources[0].shape[0]
    share = sources[0].shape[1] // shares
    f_tile = w_gate.shape[1]

    @pl.when(step == 0)
    def _():
        copies = []
        for d in range(groups):
            for j in range(shares):
                at = pl.multiple_of(jnp.bitwise_xor(t_ref[0], j) * share, share)
                copies.append(
                    pltpu.make_async_copy(
                        sources[d].at[:, pl.ds(j * share, share)],
                        rows_ref.at[pl.ds(d * rows, rows), pl.ds(at, share)],
                        sems.at[d, j],
                    )
                )
        for copy in copies:
            copy.start()
        for copy in copies:
            copy.wait()

    @pl.when(step < f_tiles)
    def _():
        gate = jnp.dot(rows_ref[...], w_gate[...], preferred_element_type=jnp.float32)
        up = jnp.dot(rows_ref[...], w_up[...], preferred_element_type=jnp.float32)
        act = (gate / (1.0 + jnp.exp(-gate)) * up).astype(jnp.bfloat16)
        if f_tile == act_ref.shape[1]:
            act_ref[...] = act
        else:
            act_ref[:, pl.ds(pl.multiple_of(step * f_tile, f_tile), f_tile)] = act

    @pl.when(step >= f_tiles)
    def _():
        out = jnp.dot(act_ref[...], w_down[...], preferred_element_type=jnp.float32)
        for d in range(groups):
            results[d][...] = out[d * rows : (d + 1) * rows]


def run_expert(sources, w_gate, w_up, w_down, tensor_index, shares):
    groups = len(sources)
    rows, width = sources[0].shape
    hidden = w_gate.shape[1]
    share = width // shares
    f_tile = tile_of(hidden, 256)
    n_tile = tile_of(share, 512)
    f_tiles, n_tiles, per = hidden // f_tile, width // n_tile, share // n_tile

    def in_tile(i, t):
        return (0, jnp.minimum(i, f_tiles - 1))

    def out_tile(i, t):
        return (0, jnp.maximum(i - f_tiles, 0))

    def down_tile(i, t):
        n = jnp.maximum(i - f_tiles, 0)
        return (0, jnp.bitwise_xor(t[0], n // per) * per + n % per)

    total = groups * rows
    return pl.pallas_call(
        functools.partial(expert_kernel, groups, shares, f_tiles),
        out_shape=[jax.ShapeDtypeStruct((rows, width), jnp.float32)] * groups,
        grid_spec=pltpu.PrefetchScalarGridSpec(
            num_scalar_prefetch=1,
            grid=(f_tiles + n_tiles,),
            in_specs=[pl.BlockSpec(memory_space=pl.ANY)] * groups
            + [
                pl.BlockSpec((width, f_tile), in_tile),
                pl.BlockSpec((width, f_tile), in_tile),
                pl.BlockSpec((hidden, n_tile), down_tile),
            ],
            out_specs=[pl.BlockSpec((rows, n_tile), out_tile)] * groups,
            scratch_shapes=[
                pltpu.VMEM((total, width), jnp.bfloat16),
                pltpu.VMEM((total, hidden), jnp.bfloat16),
                pltpu.SemaphoreType.DMA((groups, shares)),
            ],
        ),
        compiler_params=pltpu.CompilerParams(
            dimension_semantics=("arbitrary",), vmem_limit_bytes=40 << 20
        ),
        cost_estimate=pl.CostEstimate(
            flops=6 * total * width * hidden,
            bytes_accessed=6 * width * hidden + 6 * total * width,
            transcendentals=total * hidden,
        ),
        name="expert",
    )(tensor_index, *sources, w_gate, w_up, w_down)


def shards(hidden_in, expert_ids, ffn_gain, w_router, w_gate, w_up, w_down):
    tok_count = hidden_in.shape[1]
    model_width = hidden_in.shape[2]
    top_count = expert_ids.shape[2]
    expert_count = lax.axis_size("expert")
    tensor_count = lax.axis_size("tensor")
    replica_count = lax.axis_size("dp")
    experts = expert_count * w_gate.shape[0]
    capacity = max(2, 9 * tok_count * top_count // (8 * experts))
    share = model_width // tensor_count
    z = lax.axis_index("expert")
    t = lax.axis_index("tensor")
    token_rows = hidden_in.reshape(tok_count, model_width).astype(jnp.float32)
    in_squares = jnp.mean(token_rows * token_rows, axis=1)
    inverse_rms = lax.rsqrt(in_squares[:, None] + EPS_NORM)
    normed = (token_rows * inverse_rms * ffn_gain[None, :]).astype(jnp.bfloat16)
    chosen = expert_ids.reshape(tok_count, top_count)
    slot_index = slot_positions(chosen.reshape(-1), experts).reshape(tok_count, top_count)
    destination = chosen * capacity + slot_index
    slots = jnp.arange(capacity, dtype=jnp.int32)

    def own_share(array, j):
        return lax.dynamic_slice_in_dim(array, jnp.bitwise_xor(t, j) * share, share, array.ndim - 1)

    normed_shares = [own_share(normed, j) for j in range(tensor_count)]

    def picked_rows(k, j):
        row_index = jnp.bitwise_xor(z, k) * capacity + slots
        matches = jnp.any(destination[None, :, :] == row_index[:, None, None], axis=2)
        return jnp.dot(
            matches.astype(jnp.bfloat16), normed_shares[j], preferred_element_type=jnp.float32
        ).astype(jnp.bfloat16)

    half = max(1, expert_count // 2)
    chunks = [c for c in (range(half), range(half, expert_count)) if len(c)]
    tensor_index = t.astype(jnp.int32).reshape(1)
    weights_of = (w_gate[0], w_up[0], w_down[0])

    arrived = {}
    for k in range(1, expert_count):
        arrived[k] = swap(picked_rows(k, 0), "expert", k)

    results = [None] * expert_count
    for chunk in chunks:
        remote = [k for k in chunk if k]
        parts = [[arrived[k] for k in remote]]
        if remote:
            mine = jnp.concatenate(parts[0], axis=0)
            columns = [mine] + [swap(mine, "tensor", j) for j in range(1, tensor_count)]
        if chunk[0] == 0:
            local = [picked_rows(0, j) for j in range(tensor_count)]
            columns = (
                [jnp.concatenate([a, b], axis=0) for a, b in zip(local, columns)] if remote else local
            )
        rows = jnp.concatenate(columns, axis=1)
        sources = [rows] + [swap(rows, "dp", d) for d in range(1, replica_count)]
        sums = run_expert(sources, *weights_of, tensor_index, tensor_count)
        total = sums[0]
        for d in range(1, replica_count):
            total = total + swap(sums[d], "dp", d)
        owned = total[:, :share]
        for j in range(1, tensor_count):
            block = total[:, j * share : (j + 1) * share].astype(jnp.bfloat16)
            owned = owned + swap(block, "tensor", j).astype(jnp.float32)
        owned = owned.astype(jnp.bfloat16)
        for at, k in enumerate(chunk):
            block = owned[at * capacity : (at + 1) * capacity]
            results[k] = swap(block, "expert", k) if k else block

    logits = jnp.dot(normed, w_router, preferred_element_type=jnp.float32)
    selector = (chosen[:, :, None] == jnp.arange(experts, dtype=jnp.int32)[None, None, :]).astype(
        jnp.float32
    )
    picked = jnp.sum(selector * logits[:, None, :], axis=2)
    spread = picked[:, 0] - picked[:, 1]
    gate_values = jnp.stack([jax.nn.sigmoid(spread), jax.nn.sigmoid(-spread)], axis=1)
    row_index = jnp.concatenate(
        [jnp.bitwise_xor(z, k) * capacity + slots for k in range(expert_count)]
    )
    placed = (destination[:, :, None] == row_index[None, None, :]).astype(jnp.float32)
    mixing = jnp.sum(gate_values[:, :, None] * placed, axis=1)
    mixture = jnp.dot(
        mixing,
        jnp.concatenate(results, axis=0).astype(jnp.float32),
        precision=lax.Precision.HIGHEST,
    )
    own_rows = own_share(token_rows, 0)
    outputs = (own_rows + mixture).astype(jnp.bfloat16)
    out_rows = outputs.astype(jnp.float32)
    cross_sum, out_sum = lax.psum(
        (jnp.sum(own_rows * out_rows, axis=1), jnp.sum(out_rows * out_rows, axis=1)), "tensor"
    )
    cosine = (
        cross_sum
        / model_width
        * lax.rsqrt((in_squares + EPS_COS) * (out_sum / model_width + EPS_COS))
    )
    local_total = jnp.sum(1.0 - cosine)
    grand_total = lax.psum(local_total, ("expert", "dp"))
    layer_score = grand_total / (tok_count * expert_count * replica_count)
    return (outputs.reshape(1, tok_count, share), layer_score)


def solution(mesh):
    return jax.shard_map(
        shards,
        mesh=mesh,
        in_specs=(
            P("dp", "expert", None),
            P("dp", "expert", None),
            P(),
            P(),
            P("expert", None, ("tensor", "dp")),
            P("expert", None, ("tensor", "dp")),
            P("expert", ("tensor", "dp"), None),
        ),
        out_specs=(P("dp", "expert", "tensor"), P()),
        check_vma=False,
    )
```

```python
import functools
import jax
import jax.numpy as jnp
from jax import lax
from jax.experimental import pallas as pl
from jax.experimental.pallas import tpu as pltpu
from jax.sharding import PartitionSpec as P

EPS_NORM = 1e-05
EPS_COS = 1e-06
AHEAD = 2


def slot_positions(flat_ids, experts):
    pair_count = flat_ids.shape[0]
    onehot = (flat_ids[:, None] == jnp.arange(experts, dtype=jnp.int32)[None, :]).astype(jnp.int32)
    positions = jnp.arange(pair_count, dtype=jnp.int32)
    earlier = (positions[None, :] < positions[:, None]).astype(jnp.int32)
    before = jnp.sum(earlier[:, :, None] * onehot[None, :, :], axis=1)
    return jnp.sum(before * onehot, axis=1)


def swap(value, axis, step):
    count = lax.axis_size(axis)
    return lax.ppermute(value, axis, [(i, i ^ step) for i in range(count)])


def tile_of(size, most):
    for tile in range(most, 127, -128):
        if size % tile == 0:
            return tile
    return size


def expert_kernel(groups, parts, shares, f_tiles, n_tiles, t_ref, *refs):
    sources = refs[:groups]
    w_gate, w_up, w_down = refs[groups : groups + 3]
    results = refs[groups + 3 : groups + 3 + groups * len(parts)]
    (rows_ref, act_ref, out_ref, gate_buf, up_buf, down_buf) = refs[-10:-4]
    row_sems, in_sems, down_sems, out_sems = refs[-4:]
    rows = sources[0].shape[0]
    share = sources[0].shape[1] // shares
    f_tile = gate_buf.shape[2]
    n_tile = down_buf.shape[2]
    per = share // n_tile

    def row_copy(d, j):
        at = pl.multiple_of(jnp.bitwise_xor(t_ref[0], j) * share, share)
        return pltpu.make_async_copy(
            sources[d].at[:, pl.ds(j * share, share)],
            rows_ref.at[pl.ds(d * rows, rows), pl.ds(at, share)],
            row_sems.at[d, j],
        )

    def in_copy(weight, buffer, which, f):
        source = weight
        if f_tiles > 1:
            source = weight.at[:, pl.ds(pl.multiple_of(f * f_tile, f_tile), f_tile)]
        slot = lax.rem(f, gate_buf.shape[0])
        return pltpu.make_async_copy(source, buffer.at[slot], in_sems.at[which, slot])

    def down_copy(n):
        at = (jnp.bitwise_xor(t_ref[0], n // per) * per + n % per) * n_tile
        slot = lax.rem(n, down_buf.shape[0])
        return pltpu.make_async_copy(
            w_down.at[:, pl.ds(pl.multiple_of(at, n_tile), n_tile)],
            down_buf.at[slot],
            down_sems.at[slot],
        )

    def out_copies(n):
        at = pl.ds(pl.multiple_of(n * n_tile, n_tile), n_tile)
        begin = 0
        copies = []
        for which in range(groups * len(parts)):
            size = parts[which % len(parts)]
            copies.append(
                pltpu.make_async_copy(
                    out_ref.at[n, pl.ds(begin, size)],
                    results[which].at[:, at],
                    out_sems.at[which, n],
                )
            )
            begin += size
        return copies

    def start_hidden(f):
        in_copy(w_gate, gate_buf, 0, f).start()
        in_copy(w_up, up_buf, 1, f).start()

    def start_down(n):
        if isinstance(n, int):
            if n < n_tiles:
                down_copy(n).start()
        else:
            pl.when(n < n_tiles)(lambda: down_copy(n).start())

    for d in range(groups):
        for j in range(shares):
            row_copy(d, j).start()
    start_hidden(0)
    for d in range(groups):
        for j in range(shares):
            row_copy(d, j).wait()
    for f in range(1, min(AHEAD, f_tiles)):
        start_hidden(f)
    for e in range(AHEAD - f_tiles):
        start_down(2 * e)
        start_down(2 * e + 1)

    def hidden_step(f, carry):
        in_copy(w_gate, gate_buf, 0, f).wait()
        in_copy(w_up, up_buf, 1, f).wait()

        @pl.when(f + AHEAD < f_tiles)
        def _():
            start_hidden(f + AHEAD)

        @pl.when(f + AHEAD >= f_tiles)
        def _():
            start_down(2 * (f + AHEAD - f_tiles))
            start_down(2 * (f + AHEAD - f_tiles) + 1)

        slot = lax.rem(f, gate_buf.shape[0])
        gate = jnp.dot(rows_ref[...], gate_buf[slot], preferred_element_type=jnp.float32)
        up = jnp.dot(rows_ref[...], up_buf[slot], preferred_element_type=jnp.float32)
        act = (gate / (1.0 + jnp.exp(-gate)) * up).astype(jnp.bfloat16)
        if f_tiles == 1:
            act_ref[...] = act
        else:
            act_ref[:, pl.ds(pl.multiple_of(f * f_tile, f_tile), f_tile)] = act
        return carry

    def down_step(n, carry):
        down_copy(n).wait()
        start_down(n + 2 * AHEAD)
        out_ref[n] = jnp.dot(act_ref[...], down_buf[lax.rem(n, down_buf.shape[0])], preferred_element_type=jnp.float32)
        for copy in out_copies(n):
            copy.start()
        return carry

    lax.fori_loop(0, f_tiles, hidden_step, 0)
    lax.fori_loop(0, n_tiles, down_step, 0)
    for n in range(n_tiles):
        for copy in out_copies(n):
            copy.wait()


def run_expert(sources, w_gate, w_up, w_down, tensor_index, shares, parts):
    groups = len(sources)
    rows, width = sources[0].shape
    hidden = w_gate.shape[1]
    share = width // shares
    f_tile = tile_of(hidden, 256)
    n_tile = tile_of(share, 512)
    f_tiles, n_tiles = hidden // f_tile, width // n_tile
    total = groups * rows
    in_slots = min(f_tiles, AHEAD + 1)
    down_slots = min(n_tiles, 2 * AHEAD + 1)
    return pl.pallas_call(
        functools.partial(expert_kernel, groups, parts, shares, f_tiles, n_tiles),
        out_shape=[jax.ShapeDtypeStruct((size, width), jnp.float32) for size in parts] * groups,
        in_specs=[pl.BlockSpec(memory_space=pltpu.SMEM)]
        + [pl.BlockSpec(memory_space=pl.ANY)] * (groups + 3),
        out_specs=[pl.BlockSpec(memory_space=pl.ANY)] * (groups * len(parts)),
        scratch_shapes=[
            pltpu.VMEM((total, width), jnp.bfloat16),
            pltpu.VMEM((total, hidden), jnp.bfloat16),
            pltpu.VMEM((n_tiles, total, n_tile), jnp.float32),
            pltpu.VMEM((in_slots, width, f_tile), jnp.bfloat16),
            pltpu.VMEM((in_slots, width, f_tile), jnp.bfloat16),
            pltpu.VMEM((down_slots, hidden, n_tile), jnp.bfloat16),
            pltpu.SemaphoreType.DMA((groups, shares)),
            pltpu.SemaphoreType.DMA((2, in_slots)),
            pltpu.SemaphoreType.DMA((down_slots,)),
            pltpu.SemaphoreType.DMA((groups * len(parts), n_tiles)),
        ],
        compiler_params=pltpu.CompilerParams(vmem_limit_bytes=38 << 20),
        cost_estimate=pl.CostEstimate(
            flops=6 * total * width * hidden,
            bytes_accessed=6 * width * hidden + 6 * total * width,
            transcendentals=total * hidden,
        ),
        name="expert",
    )(tensor_index, *sources, w_gate, w_up, w_down)


def sum_over(value, axis):
    step = 1
    while step < lax.axis_size(axis):
        value = value + swap(value, axis, step)
        step *= 2
    return value


def shards(hidden_in, expert_ids, ffn_gain, w_router, w_gate, w_up, w_down):
    tok_count = hidden_in.shape[1]
    model_width = hidden_in.shape[2]
    top_count = expert_ids.shape[2]
    expert_count = lax.axis_size("expert")
    tensor_count = lax.axis_size("tensor")
    replica_count = lax.axis_size("dp")
    experts = expert_count * w_gate.shape[0]
    capacity = max(2, 9 * tok_count * top_count // (8 * experts))
    share = model_width // tensor_count
    z = lax.axis_index("expert")
    t = lax.axis_index("tensor")
    token_rows = hidden_in.reshape(tok_count, model_width).astype(jnp.float32)
    in_squares = jnp.mean(token_rows * token_rows, axis=1)
    inverse_rms = lax.rsqrt(in_squares[:, None] + EPS_NORM)
    normed = (token_rows * inverse_rms * ffn_gain[None, :]).astype(jnp.bfloat16)
    chosen = expert_ids.reshape(tok_count, top_count)
    slot_index = slot_positions(chosen.reshape(-1), experts).reshape(tok_count, top_count)
    destination = chosen * capacity + slot_index
    slots = jnp.arange(capacity, dtype=jnp.int32)

    def own_share(array, j):
        return lax.dynamic_slice_in_dim(array, jnp.bitwise_xor(t, j) * share, share, array.ndim - 1)

    normed_shares = [own_share(normed, j) for j in range(tensor_count)]

    def picked_rows(k, j):
        row_index = jnp.bitwise_xor(z, k) * capacity + slots
        matches = jnp.any(destination[None, :, :] == row_index[:, None, None], axis=2)
        return jnp.dot(
            matches.astype(jnp.bfloat16), normed_shares[j], preferred_element_type=jnp.float32
        ).astype(jnp.bfloat16)

    half = max(1, expert_count // 2)
    chunks = [c for c in (range(half), range(half, expert_count)) if len(c)]
    tensor_index = t.astype(jnp.int32).reshape(1)
    weights_of = (w_gate[0], w_up[0], w_down[0])

    arrived = {}
    for chunk in chunks:
        for k in chunk:
            if k:
                arrived[k] = swap(picked_rows(k, 0), "expert", k)

    results = [None] * expert_count
    for number, chunk in enumerate(chunks):
        remote = [k for k in chunk if k]
        if remote:
            mine = jnp.concatenate([arrived[k] for k in remote], axis=0)
            columns = [mine] + [swap(mine, "tensor", j) for j in range(1, tensor_count)]
        if chunk[0] == 0:
            local = [picked_rows(0, j) for j in range(tensor_count)]
        if chunk[0] == 0:
            columns = [
                jnp.concatenate([a, b], axis=0) if remote else a
                for a, b in zip(local, columns if remote else local)
            ]
        rows = jnp.concatenate(columns, axis=1)
        sources = [rows] + [swap(rows, "dp", d) for d in range(1, replica_count)]
        split = number and capacity % 8 == 0
        parts = [[k] for k in chunk] if split else [list(chunk)]
        sums = run_expert(
            sources,
            *weights_of,
            tensor_index,
            tensor_count,
            [capacity * len(part) for part in parts],
        )
        for at, part in enumerate(parts):
            total = sums[at]
            for d in range(1, replica_count):
                total = total + swap(sums[d * len(parts) + at], "dp", d)
            owned = total[:, :share]
            for j in range(1, tensor_count):
                block = total[:, j * share : (j + 1) * share].astype(jnp.bfloat16)
                owned = owned + swap(block, "tensor", j).astype(jnp.float32)
            owned = owned.astype(jnp.bfloat16)
            for i, k in enumerate(part):
                block = owned[i * capacity : (i + 1) * capacity]
                results[k] = swap(block, "expert", k) if k else block

    logits = jnp.dot(normed, w_router, preferred_element_type=jnp.float32)
    selector = (chosen[:, :, None] == jnp.arange(experts, dtype=jnp.int32)[None, None, :]).astype(
        jnp.float32
    )
    picked = jnp.sum(selector * logits[:, None, :], axis=2)
    spread = picked[:, 0] - picked[:, 1]
    gate_values = jnp.stack([jax.nn.sigmoid(spread), jax.nn.sigmoid(-spread)], axis=1)
    row_index = jnp.concatenate(
        [jnp.bitwise_xor(z, k) * capacity + slots for k in range(expert_count)]
    )
    placed = (destination[:, :, None] == row_index[None, None, :]).astype(jnp.float32)
    mixing = jnp.sum(gate_values[:, :, None] * placed, axis=1)
    mixture = jnp.dot(
        mixing,
        jnp.concatenate(results, axis=0).astype(jnp.float32),
        precision=lax.Precision.HIGHEST,
    )
    own_rows = own_share(token_rows, 0)
    outputs = (own_rows + mixture).astype(jnp.bfloat16)
    out_rows = outputs.astype(jnp.float32)
    partial = jnp.stack([jnp.sum(own_rows * out_rows, axis=1), jnp.sum(out_rows * out_rows, axis=1)])
    cross_sum, out_sum = sum_over(partial, "tensor")
    cosine = (
        cross_sum
        / model_width
        * lax.rsqrt((in_squares + EPS_COS) * (out_sum / model_width + EPS_COS))
    )
    local_total = jnp.sum(1.0 - cosine)
    grand_total = sum_over(sum_over(local_total.reshape(1), "dp"), "expert")
    layer_score = grand_total[0] / (tok_count * expert_count * replica_count)
    return (outputs.reshape(1, tok_count, share), layer_score)


def solution(mesh):
    return jax.shard_map(
        shards,
        mesh=mesh,
        in_specs=(
            P("dp", "expert", None),
            P("dp", "expert", None),
            P(),
            P(),
            P("expert", None, ("tensor", "dp")),
            P("expert", None, ("tensor", "dp")),
            P("expert", ("tensor", "dp"), None),
        ),
        out_specs=(P("dp", "expert", "tensor"), P()),
        check_vma=False,
    )
```

```python
import functools
import jax
import jax.numpy as jnp
from jax import lax
from jax.experimental import pallas as pl
from jax.experimental.pallas import tpu as pltpu
from jax.sharding import PartitionSpec as P

EPS_NORM = 1e-05
EPS_COS = 1e-06
AHEAD = 2


def slot_positions(flat_ids, experts):
    pair_count = flat_ids.shape[0]
    onehot = (flat_ids[:, None] == jnp.arange(experts, dtype=jnp.int32)[None, :]).astype(jnp.int32)
    positions = jnp.arange(pair_count, dtype=jnp.int32)
    earlier = (positions[None, :] < positions[:, None]).astype(jnp.int32)
    before = jnp.sum(earlier[:, :, None] * onehot[None, :, :], axis=1)
    return jnp.sum(before * onehot, axis=1)


def swap(value, axis, step):
    count = lax.axis_size(axis)
    return lax.ppermute(value, axis, [(i, i ^ step) for i in range(count)])


def tile_of(size, most):
    for tile in range(most, 127, -128):
        if size % tile == 0:
            return tile
    return size


def hidden_kernel(groups, shares, f_tiles, t_ref, *refs):
    sources = refs[:groups]
    w_gate, w_up, act_ref, rows_ref, gate_buf, up_buf, row_sems, in_sems = refs[groups:]
    rows = sources[0].shape[0]
    share = sources[0].shape[1] // shares
    slots, _, f_tile = gate_buf.shape

    def row_copies():
        copies = []
        for d in range(groups):
            for j in range(shares):
                at = pl.multiple_of(jnp.bitwise_xor(t_ref[0], j) * share, share)
                copies.append(
                    pltpu.make_async_copy(
                        sources[d].at[:, pl.ds(j * share, share)],
                        rows_ref.at[pl.ds(d * rows, rows), pl.ds(at, share)],
                        row_sems.at[d, j],
                    )
                )
        return copies

    def in_copies(f):
        slot = lax.rem(f, slots)
        at = pl.ds(pl.multiple_of(f * f_tile, f_tile), f_tile)
        pairs = ((w_gate, gate_buf), (w_up, up_buf))
        return [
            pltpu.make_async_copy(
                weight.at[:, at] if f_tiles > 1 else weight, buffer.at[slot], in_sems.at[i, slot]
            )
            for i, (weight, buffer) in enumerate(pairs)
        ]

    def start_in(f):
        for copy in in_copies(f):
            copy.start()

    for copy in row_copies():
        copy.start()
    start_in(0)
    for copy in row_copies():
        copy.wait()
    for f in range(1, min(AHEAD, f_tiles)):
        start_in(f)

    def step(f, carry):
        for copy in in_copies(f):
            copy.wait()
        pl.when(f + AHEAD < f_tiles)(lambda: start_in(f + AHEAD))
        slot = lax.rem(f, slots)
        gate = jnp.dot(rows_ref[...], gate_buf[slot], preferred_element_type=jnp.float32)
        up = jnp.dot(rows_ref[...], up_buf[slot], preferred_element_type=jnp.float32)
        act = (gate / (1.0 + jnp.exp(-gate)) * up).astype(jnp.bfloat16)
        if f_tiles == 1:
            act_ref[...] = act
        else:
            act_ref[:, pl.ds(pl.multiple_of(f * f_tile, f_tile), f_tile)] = act
        return carry

    lax.fori_loop(0, f_tiles, step, 0)


def down_kernel(parts, shares, n_tiles, t_ref, act_ref, w_down, *refs):
    results = refs[: len(parts)]
    out_ref, down_buf, down_sems, out_sems = refs[len(parts) :]
    slots, _, n_tile = down_buf.shape
    per = n_tiles // shares

    def down_copy(n):
        at = (jnp.bitwise_xor(t_ref[0], n // per) * per + lax.rem(n, per)) * n_tile
        slot = lax.rem(n, slots)
        return pltpu.make_async_copy(
            w_down.at[:, pl.ds(pl.multiple_of(at, n_tile), n_tile)],
            down_buf.at[slot],
            down_sems.at[slot],
        )

    def out_copies(n):
        at = pl.ds(pl.multiple_of(n * n_tile, n_tile), n_tile)
        begin = 0
        copies = []
        for which, size in enumerate(parts):
            copies.append(
                pltpu.make_async_copy(
                    out_ref.at[n, pl.ds(begin, size)],
                    results[which].at[:, at],
                    out_sems.at[which, n],
                )
            )
            begin += size
        return copies

    for n in range(slots - 1):
        down_copy(n).start()

    def step(n, carry):
        down_copy(n).wait()
        pl.when(n + slots - 1 < n_tiles)(lambda: down_copy(n + slots - 1).start())
        out_ref[n] = jnp.dot(
            act_ref[...], down_buf[lax.rem(n, slots)], preferred_element_type=jnp.float32
        )
        for copy in out_copies(n):
            copy.start()
        return carry

    lax.fori_loop(0, n_tiles, step, 0)
    for n in range(n_tiles):
        for copy in out_copies(n):
            copy.wait()


def run_hidden(sources, w_gate, w_up, tensor_index, shares):
    groups = len(sources)
    rows, width = sources[0].shape
    hidden = w_gate.shape[1]
    f_tile = tile_of(hidden, 256)
    f_tiles = hidden // f_tile
    total = groups * rows
    slots = min(f_tiles, AHEAD + 1)
    return pl.pallas_call(
        functools.partial(hidden_kernel, groups, shares, f_tiles),
        out_shape=jax.ShapeDtypeStruct((total, hidden), jnp.bfloat16),
        in_specs=[pl.BlockSpec(memory_space=pltpu.SMEM)]
        + [pl.BlockSpec(memory_space=pl.ANY)] * (groups + 2),
        out_specs=pl.BlockSpec(memory_space=pltpu.VMEM),
        scratch_shapes=[
            pltpu.VMEM((total, width), jnp.bfloat16),
            pltpu.VMEM((slots, width, f_tile), jnp.bfloat16),
            pltpu.VMEM((slots, width, f_tile), jnp.bfloat16),
            pltpu.SemaphoreType.DMA((groups, shares)),
            pltpu.SemaphoreType.DMA((2, slots)),
        ],
        compiler_params=pltpu.CompilerParams(vmem_limit_bytes=44 << 20),
        cost_estimate=pl.CostEstimate(
            flops=4 * total * width * hidden,
            bytes_accessed=4 * width * hidden + 2 * total * (width + hidden),
            transcendentals=total * hidden,
        ),
        name="hidden",
    )(tensor_index, *sources, w_gate, w_up)


def run_down(act, w_down, tensor_index, shares, parts):
    total, hidden = act.shape
    width = w_down.shape[1]
    n_tile = tile_of(width // shares, 512)
    n_tiles = width // n_tile
    slots = min(n_tiles, 2 * AHEAD + 1)
    return pl.pallas_call(
        functools.partial(down_kernel, parts, shares, n_tiles),
        out_shape=[jax.ShapeDtypeStruct((size, width), jnp.float32) for size in parts],
        in_specs=[
            pl.BlockSpec(memory_space=pltpu.SMEM),
            pl.BlockSpec(memory_space=pltpu.VMEM),
            pl.BlockSpec(memory_space=pl.ANY),
        ],
        out_specs=[pl.BlockSpec(memory_space=pl.ANY)] * len(parts),
        scratch_shapes=[
            pltpu.VMEM((n_tiles, total, n_tile), jnp.float32),
            pltpu.VMEM((slots, hidden, n_tile), jnp.bfloat16),
            pltpu.SemaphoreType.DMA((slots,)),
            pltpu.SemaphoreType.DMA((len(parts), n_tiles)),
        ],
        compiler_params=pltpu.CompilerParams(vmem_limit_bytes=44 << 20),
        cost_estimate=pl.CostEstimate(
            flops=2 * total * width * hidden,
            bytes_accessed=2 * width * hidden + 2 * total * hidden + 4 * total * width,
            transcendentals=0,
        ),
        name="down",
    )(tensor_index, act, w_down)


def sum_over(value, axis):
    step = 1
    while step < lax.axis_size(axis):
        value = value + swap(value, axis, step)
        step *= 2
    return value


def shards(hidden_in, expert_ids, ffn_gain, w_router, w_gate, w_up, w_down):
    tok_count = hidden_in.shape[1]
    model_width = hidden_in.shape[2]
    top_count = expert_ids.shape[2]
    expert_count = lax.axis_size("expert")
    tensor_count = lax.axis_size("tensor")
    replica_count = lax.axis_size("dp")
    experts = expert_count * w_gate.shape[0]
    capacity = max(2, 9 * tok_count * top_count // (8 * experts))
    share = model_width // tensor_count
    z = lax.axis_index("expert")
    t = lax.axis_index("tensor")
    token_rows = hidden_in.reshape(tok_count, model_width).astype(jnp.float32)
    in_squares = jnp.mean(token_rows * token_rows, axis=1)
    inverse_rms = lax.rsqrt(in_squares[:, None] + EPS_NORM)
    normed = (token_rows * inverse_rms * ffn_gain[None, :]).astype(jnp.bfloat16)
    chosen = expert_ids.reshape(tok_count, top_count)
    slot_index = slot_positions(chosen.reshape(-1), experts).reshape(tok_count, top_count)
    destination = chosen * capacity + slot_index
    slots = jnp.arange(capacity, dtype=jnp.int32)

    def own_share(array, j):
        return lax.dynamic_slice_in_dim(array, jnp.bitwise_xor(t, j) * share, share, array.ndim - 1)

    normed_shares = [own_share(normed, j) for j in range(tensor_count)]

    def picked_rows(k, j):
        row_index = jnp.bitwise_xor(z, k) * capacity + slots
        matches = jnp.any(destination[None, :, :] == row_index[:, None, None], axis=2)
        return jnp.dot(
            matches.astype(jnp.bfloat16), normed_shares[j], preferred_element_type=jnp.float32
        ).astype(jnp.bfloat16)

    half = max(1, expert_count // 2)
    chunks = [c for c in (range(half), range(half, expert_count)) if len(c)]
    tensor_index = t.astype(jnp.int32).reshape(1)

    arrived = {}
    for chunk in chunks:
        for k in chunk:
            if k:
                arrived[k] = swap(picked_rows(k, 0), "expert", k)

    results = [None] * expert_count
    for number, chunk in enumerate(chunks):
        remote = [k for k in chunk if k]
        if remote:
            mine = jnp.concatenate([arrived[k] for k in remote], axis=0)
            columns = [mine] + [swap(mine, "tensor", j) for j in range(1, tensor_count)]
        if chunk[0] == 0:
            local = [picked_rows(0, j) for j in range(tensor_count)]
        if chunk[0] == 0:
            columns = [
                jnp.concatenate([a, b], axis=0) if remote else a
                for a, b in zip(local, columns if remote else local)
            ]
        rows = jnp.concatenate(columns, axis=1)
        sources = [rows] + [swap(rows, "dp", d) for d in range(1, replica_count)]
        split = number and capacity % 8 == 0
        parts = [[k] for k in chunk] if split else [list(chunk)]
        act = run_hidden(sources, w_gate[0], w_up[0], tensor_index, tensor_count)
        sums = run_down(
            act,
            w_down[0],
            tensor_index,
            tensor_count,
            [capacity * len(part) for part in parts] * replica_count,
        )
        for at, part in enumerate(parts):
            total = sums[at]
            for d in range(1, replica_count):
                total = total + swap(sums[d * len(parts) + at], "dp", d)
            owned = total[:, :share]
            for j in range(1, tensor_count):
                block = total[:, j * share : (j + 1) * share].astype(jnp.bfloat16)
                owned = owned + swap(block, "tensor", j).astype(jnp.float32)
            owned = owned.astype(jnp.bfloat16)
            for i, k in enumerate(part):
                block = owned[i * capacity : (i + 1) * capacity]
                results[k] = swap(block, "expert", k) if k else block

    logits = jnp.dot(normed, w_router, preferred_element_type=jnp.float32)
    selector = (chosen[:, :, None] == jnp.arange(experts, dtype=jnp.int32)[None, None, :]).astype(
        jnp.float32
    )
    picked = jnp.sum(selector * logits[:, None, :], axis=2)
    spread = picked[:, 0] - picked[:, 1]
    gate_values = jnp.stack([jax.nn.sigmoid(spread), jax.nn.sigmoid(-spread)], axis=1)
    row_index = jnp.concatenate(
        [jnp.bitwise_xor(z, k) * capacity + slots for k in range(expert_count)]
    )
    placed = (destination[:, :, None] == row_index[None, None, :]).astype(jnp.float32)
    mixing = jnp.sum(gate_values[:, :, None] * placed, axis=1)
    mixture = jnp.dot(
        mixing,
        jnp.concatenate(results, axis=0).astype(jnp.float32),
        precision=lax.Precision.HIGHEST,
    )
    own_rows = own_share(token_rows, 0)
    outputs = (own_rows + mixture).astype(jnp.bfloat16)
    out_rows = outputs.astype(jnp.float32)
    partial = jnp.stack([jnp.sum(own_rows * out_rows, axis=1), jnp.sum(out_rows * out_rows, axis=1)])
    cross_sum, out_sum = sum_over(partial, "tensor")
    cosine = (
        cross_sum
        / model_width
        * lax.rsqrt((in_squares + EPS_COS) * (out_sum / model_width + EPS_COS))
    )
    local_total = jnp.sum(1.0 - cosine)
    grand_total = sum_over(sum_over(local_total.reshape(1), "dp"), "expert")
    layer_score = grand_total[0] / (tok_count * expert_count * replica_count)
    return (outputs.reshape(1, tok_count, share), layer_score)


def solution(mesh):
    return jax.shard_map(
        shards,
        mesh=mesh,
        in_specs=(
            P("dp", "expert", None),
            P("dp", "expert", None),
            P(),
            P(),
            P("expert", None, ("tensor", "dp")),
            P("expert", None, ("tensor", "dp")),
            P("expert", ("tensor", "dp"), None),
        ),
        out_specs=(P("dp", "expert", "tensor"), P()),
        check_vma=False,
    )
```
